32 devices in a mesh: fsdp: 16 (over z, y, core), tp: 2 (over x).
Axes of the slice: x: 2, y: 2, z: 4, core: 2. Of those that a mesh axis runs over, the one named last changes fastest.
Arguments:
- hidden: bfloat16 [32, 5120], P(None, 'fsdp'), may hold values from -20 to 20
- query_weight: bfloat16 [5120, 5120], P(None, ('tp', 'fsdp')), may hold values from -0.078125 to 0.078125
- key_weight: bfloat16 [5120, 1024], P(None, ('tp', 'fsdp')), may hold values from -0.078125 to 0.078125
- value_weight: bfloat16 [5120, 1024], P(None, ('tp', 'fsdp')), may hold values from -0.078125 to 0.078125
- output_weight: bfloat16 [5120, 5120], P(('tp', 'fsdp')), may hold values from -0.078125 to 0.078125
- gate_weight: bfloat16 [5120, 27648], P(None, ('tp', 'fsdp')), may hold values from -0.078125 to 0.078125
- up_weight: bfloat16 [5120, 27648], P(None, ('tp', 'fsdp')), may hold values from -0.078125 to 0.078125
- down_weight: bfloat16 [27648, 5120], P(('tp', 'fsdp')), may hold values from -0.0390625 to 0.0390625
- history: float32 [7, 1024], replicated, may hold values from 0.0001 to 1, as said below
- slot: int32 [1], replicated, may hold values from 0 to 1023
- lengths: int32 [32], P('fsdp'), may hold values from 512 to 4096, as said below
- key_cache: bfloat16 [32, 4096, 1024], P('fsdp', None, 'tp'), may hold values from -1000 to 1000
- value_cache: bfloat16 [32, 4096, 1024], P('fsdp', None, 'tp'), may hold values from -6 to 6
Outputs:
- attention_out: bfloat16 [32, 5120], P('fsdp', 'tp')
- query_rollout: bfloat16 [5120, 5120], P('fsdp', 'tp')
- key_rollout: bfloat16 [5120, 1024], P('fsdp', 'tp')
- value_rollout: bfloat16 [5120, 1024], P('fsdp', 'tp')
- output_rollout: bfloat16 [5120, 5120], P('tp', 'fsdp')
- gate_rollout: bfloat16 [5120, 27648], P('fsdp', 'tp')
- up_rollout: bfloat16 [5120, 27648], P('fsdp', 'tp')
- down_rollout: bfloat16 [27648, 5120], P('tp', 'fsdp')
- new_history: float32 [7, 1024], replicated
The draws below stay inside these ranges and needn't reach their ends.
Inputs may be any that keep to these rules, and one draw needn't show every extreme that they name: `history`: strictly positive. `lengths`: some sequence has all 4096 slots valid.
All inputs are finite; a program needn't handle non-finite values.
Results may differ from the reference program's by a relative error of at most 0.012.
The reference program's roundings to bfloat16 on the way (of `probs`) count: a program that leaves them out, or rounds other values in their place, can miss the bound.
Values may be sent and summed in bfloat16 or wider, within the bound.
No kernel may reach another device: no remote copies, remote signals or barrier semaphores. Data moves between devices by JAX's collectives and lax.ppermute only.
A program may use at most 192 MiB of HBM per device.

```python
import jax
import jax.numpy as jnp
from jax import lax

D = 5120
F = 27648
HEADS = 40
KV_HEADS = 8
HEAD_DIM = 128
HIST = 1024
CACHE = 4096
SEQS = 32


def draw_hidden(key, part):
    values = jnp.clip(jax.random.normal(jax.random.fold_in(key, 11), (SEQS, D), jnp.float32), -6.0, 6.0)
    return values.astype(jnp.bfloat16)


def draw_history(key, part):
    fans = jnp.array([D, D, D, D, D, D, F], jnp.float32)
    low, high = (3.0, 12.0)
    levels = jnp.exp(jax.random.uniform(jax.random.fold_in(key, 21), (7,), jnp.float32, jnp.log(low), jnp.log(high)))
    spread = jnp.exp(jax.random.uniform(jax.random.fold_in(key, 22), (7, HIST), jnp.float32, jnp.log(0.02), 0.0))
    return (fans ** (-0.5) * levels)[:, None] * spread


def draw_lengths(key, part):
    counts = jax.random.randint(jax.random.fold_in(key, 31), (SEQS,), CACHE // 8, CACHE + 1)
    chosen = jax.random.randint(jax.random.fold_in(key, 32), (), 0, SEQS)
    return jnp.where(jnp.arange(SEQS) == chosen, CACHE, counts).astype(jnp.int32)


def draw_key_cache(key, part):
    values = jnp.clip(jax.random.normal(jax.random.fold_in(key, 41), (SEQS, CACHE, KV_HEADS * HEAD_DIM), jnp.float32), -6.0, 6.0)
    return values.astype(jnp.bfloat16)


def block_scale(own_key, shape, cuts, low, top_value):
    level, own = 1.0, jax.random.fold_in(own_key, 6)
    for dim, shards_of in cuts:
        heights = jnp.exp(jax.random.uniform(jax.random.fold_in(own, dim), (shards_of,), jnp.float32, low / len(cuts), top_value / len(cuts)))
        level = level * jnp.repeat(heights, shape[dim] // shards_of).reshape([-1 if axis == dim else 1 for axis in range(len(shape))])
    return level


def scatter_about(rng, extent, width, reach, cuts=(), kind=jnp.bfloat16):
    loudness = block_scale(rng, extent, cuts, -0.22, 0.18) if cuts else 1.0
    values = jax.random.normal(rng, extent, jnp.float32) * width * loudness
    return jnp.minimum(jnp.maximum(values, -reach), reach).astype(kind)


def setup_inputs(seed: int = 0) -> dict:
    streams_of = jax.random.split(jax.random.key(seed), 14)
    hidden = draw_hidden(jax.random.fold_in(streams_of[13], 71), 0)
    query_weight = scatter_about(streams_of[1], (D, D), D ** -0.5, 0.078125, ((1, 32),))
    key_weight = scatter_about(streams_of[2], (D, KV_HEADS * HEAD_DIM), D ** -0.5, 0.078125, ((1, 32),))
    value_weight = scatter_about(streams_of[3], (D, KV_HEADS * HEAD_DIM), D ** -0.5, 0.078125, ((1, 32),))
    output_weight = scatter_about(streams_of[4], (D, D), D ** -0.5, 0.078125, ((0, 32),))
    gate_weight = scatter_about(streams_of[5], (D, F), D ** -0.5, 0.078125, ((1, 32),))
    up_weight = scatter_about(streams_of[6], (D, F), D ** -0.5, 0.078125, ((1, 32),))
    down_weight = scatter_about(streams_of[7], (F, D), F ** -0.5, 0.0390625, ((0, 32),))
    history = draw_history(jax.random.fold_in(streams_of[13], 71), 0)
    slot = jax.random.randint(streams_of[9], (1,), 0, HIST).astype(jnp.int32)
    lengths = draw_lengths(jax.random.fold_in(streams_of[13], 71), 0)
    key_cache = draw_key_cache(jax.random.fold_in(streams_of[13], 71), 0)
    value_cache = scatter_about(streams_of[12], (SEQS, CACHE, KV_HEADS * HEAD_DIM), 1.0, 6.0, ((0, 16), (2, 2)))
    return dict(hidden=hidden, query_weight=query_weight, key_weight=key_weight, value_weight=value_weight, output_weight=output_weight, gate_weight=gate_weight, up_weight=up_weight, down_weight=down_weight, history=history, slot=slot, lengths=lengths, key_cache=key_cache, value_cache=value_cache)


target_peak = 4.0
norm_eps = 1e-06
rope_theta = 1000000.0

def largest(tensor):
    return jnp.max(jnp.abs(tensor.astype(jnp.float32)))

def scaling(peaks, history, slot):
    marked = lax.broadcasted_iota(jnp.int32, history.shape, 1) == slot[0]
    kept = lax.optimization_barrier(jnp.max(jnp.where(marked, jnp.zeros_like(history), history), axis=1))
    return (target_peak / jnp.maximum(peaks, kept), jnp.where(marked, peaks[:, None], history))

def quantize(tensor, factor):
    return (tensor.astype(jnp.float32) * factor).astype(jnp.bfloat16)

def rotate(vectors, positions):
    half_dim = vectors.shape[-1] // 2
    ladder = jnp.arange(half_dim, dtype=jnp.float32)
    spread = rope_theta ** (-2.0 * ladder / vectors.shape[-1])
    angle = positions.astype(jnp.float32)[:, None] * spread[None, :]
    cosine = jnp.cos(angle)[:, None, :]
    sine = jnp.sin(angle)[:, None, :]
    first = vectors[..., :half_dim]
    second = vectors[..., half_dim:]
    return jnp.concatenate([first * cosine - second * sine, second * cosine + first * sine], axis=-1)

def one_sequence(items):
    query, key_new, value_new, cached_keys, cached_values, length = items
    kv_count = query.shape[0]
    head_dim = query.shape[2]
    cache_len = cached_keys.shape[0]
    keys = cached_keys.reshape(cache_len, kv_count, head_dim).astype(jnp.float32)
    values = cached_values.reshape(cache_len, kv_count, head_dim).astype(jnp.float32)
    scale = head_dim ** (-0.5)
    widened = query.astype(jnp.float32)
    scores = jnp.einsum('kgd,jkd->kgj', widened, keys) * scale
    own = lax.optimization_barrier(jnp.sum(widened * key_new.astype(jnp.float32)[:, None, :], axis=-1)) * scale
    valid = (lax.broadcasted_iota(jnp.int32, (cache_len,), 0) < length)[None, None, :]
    top = jnp.maximum(lax.optimization_barrier(jnp.max(jnp.where(valid, scores, -1e+30), axis=-1)), own)
    weights = jnp.where(valid, jnp.exp(scores - top[..., None]), 0.0)
    own_weight = jnp.exp(own - top)
    total = lax.optimization_barrier(jnp.sum(weights, axis=-1)) + own_weight
    probs = (weights / total[..., None]).astype(jnp.bfloat16)
    own_prob = (own_weight / total).astype(jnp.bfloat16)
    mixed = jnp.einsum('kgj,jkd->kgd', probs.astype(jnp.float32), values)
    mixed = mixed + own_prob.astype(jnp.float32)[..., None] * value_new.astype(jnp.float32)[:, None, :]
    return mixed.astype(jnp.bfloat16).reshape(-1)

def reference(hidden, query_weight, key_weight, value_weight, output_weight, gate_weight, up_weight, down_weight, history, slot, lengths, key_cache, value_cache):
    trainer = [query_weight, key_weight, value_weight, output_weight, gate_weight, up_weight, down_weight]
    peaks = jnp.stack([largest(tensor) for tensor in trainer])
    factors, new_history = scaling(peaks, history, slot)
    rollout = [quantize(trainer[number], factors[number]) for number in range(7)]
    widened = hidden.astype(jnp.float32)
    inv_rms = lax.rsqrt(lax.optimization_barrier(jnp.mean(widened * widened, axis=1)) + norm_eps)[:, None]
    query = jnp.dot(hidden, rollout[0], preferred_element_type=jnp.float32) * inv_rms / factors[0]
    key_new = jnp.dot(hidden, rollout[1], preferred_element_type=jnp.float32) * inv_rms / factors[1]
    value_new = jnp.dot(hidden, rollout[2], preferred_element_type=jnp.float32) * inv_rms / factors[2]
    count_seq = hidden.shape[0]
    query = rotate(query.reshape(count_seq, HEADS, HEAD_DIM), lengths).astype(jnp.bfloat16)
    query = query.reshape(count_seq, KV_HEADS, HEADS // KV_HEADS, HEAD_DIM)
    key_new = rotate(key_new.reshape(count_seq, KV_HEADS, HEAD_DIM), lengths).astype(jnp.bfloat16)
    value_new = value_new.reshape(count_seq, KV_HEADS, HEAD_DIM).astype(jnp.bfloat16)
    attention_out = lax.map(one_sequence, (query, key_new, value_new, key_cache, value_cache, lengths))
    return (attention_out, rollout[0], rollout[1], rollout[2], rollout[3], rollout[4], rollout[5], rollout[6], new_history)
```

```python
import functools

import jax
import jax.numpy as jnp
from jax import lax
from jax.experimental import pallas as pl
from jax.experimental.pallas import tpu as pltpu
from jax.sharding import PartitionSpec as P


D = 5120
HEADS = 40
KV_HEADS = 8
HEAD_DIM = 128


target_peak = 4.0
norm_eps = 1e-06
rope_theta = 1000000.0


def largest(tensor):
    return jnp.max(jnp.abs(tensor.astype(jnp.float32)))


def scaling(peaks, history, slot):
    marked = lax.broadcasted_iota(jnp.int32, history.shape, 1) == slot[0]
    kept = jnp.max(jnp.where(marked, jnp.zeros_like(history), history), axis=1)
    return (target_peak / jnp.maximum(peaks, kept), jnp.where(marked, peaks[:, None], history))


def quantize(tensor, factor):
    return (tensor.astype(jnp.float32) * factor).astype(jnp.bfloat16)


def rotate(vectors, positions):
    half_dim = vectors.shape[-1] // 2
    ladder = jnp.arange(half_dim, dtype=jnp.float32)
    spread = rope_theta ** (-2.0 * ladder / vectors.shape[-1])
    angle = positions.astype(jnp.float32)[:, None] * spread[None, :]
    cosine = jnp.cos(angle)[:, None, :]
    sine = jnp.sin(angle)[:, None, :]
    first = vectors[..., :half_dim]
    second = vectors[..., half_dim:]
    return jnp.concatenate(
        [first * cosine - second * sine, second * cosine + first * sine], axis=-1
    )


def regroup(query_part, key_part, value_part, output_part, gate_part, up_part, down_part):
    columns = (
        lax.all_to_all(query_part, "fsdp", split_axis=0, concat_axis=1, tiled=True),
        lax.all_to_all(key_part, "fsdp", split_axis=0, concat_axis=1, tiled=True),
        lax.all_to_all(value_part, "fsdp", split_axis=0, concat_axis=1, tiled=True),
        lax.all_to_all(gate_part, "fsdp", split_axis=0, concat_axis=1, tiled=True),
        lax.all_to_all(up_part, "fsdp", split_axis=0, concat_axis=1, tiled=True),
    )
    rowwise = (
        lax.all_to_all(output_part, "fsdp", split_axis=1, concat_axis=0, tiled=True),
        lax.all_to_all(down_part, "fsdp", split_axis=1, concat_axis=0, tiled=True),
    )
    return (columns[0], columns[1], columns[2], rowwise[0], columns[3], columns[4], rowwise[1])


def attend(query, key_new, value_new, key_cache, value_cache, lengths):
    count_seq = query.shape[0]
    kv_count = query.shape[1]
    head_dim = query.shape[3]
    cache_len = key_cache.shape[1]
    keys = key_cache.reshape(count_seq, cache_len, kv_count, head_dim)
    values = value_cache.reshape(count_seq, cache_len, kv_count, head_dim)
    scale = head_dim ** (-0.5)
    scores = jnp.einsum("bkgd,bjkd->bkgj", query, keys, preferred_element_type=jnp.float32) * scale
    own = (
        jnp.sum(query.astype(jnp.float32) * key_new.astype(jnp.float32)[:, :, None, :], axis=-1)
        * scale
    )
    valid = (lax.broadcasted_iota(jnp.int32, (count_seq, cache_len), 1) < lengths[:, None])[
        :, None, None, :
    ]
    top = jnp.maximum(jnp.max(jnp.where(valid, scores, -1e30), axis=-1), own)
    weights = jnp.where(valid, jnp.exp(scores - top[..., None]), 0.0)
    own_weight = jnp.exp(own - top)
    total = jnp.sum(weights, axis=-1) + own_weight
    probs = (weights / total[..., None]).astype(jnp.bfloat16)
    own_prob = (own_weight / total).astype(jnp.bfloat16)
    mixed = jnp.einsum("bkgj,bjkd->bkgd", probs, values, preferred_element_type=jnp.float32)
    mixed = (
        mixed
        + own_prob.astype(jnp.float32)[..., None] * value_new.astype(jnp.float32)[:, :, None, :]
    )
    return mixed.astype(jnp.bfloat16).reshape(count_seq, -1)


def general_step(
    hidden,
    query_weight,
    key_weight,
    value_weight,
    output_weight,
    gate_weight,
    up_weight,
    down_weight,
    history,
    slot,
    lengths,
    key_cache,
    value_cache,
):
    trainer = (
        query_weight,
        key_weight,
        value_weight,
        output_weight,
        gate_weight,
        up_weight,
        down_weight,
    )
    peaks = jnp.stack([lax.pmax(largest(tensor), ("fsdp", "tp")) for tensor in trainer])
    factors, new_history = scaling(peaks, history, slot)
    arrived = regroup(
        query_weight, key_weight, value_weight, output_weight, gate_weight, up_weight, down_weight
    )
    rollout = tuple((quantize(arrived[number], factors[number]) for number in range(7)))
    (
        query_rollout,
        key_rollout,
        value_rollout,
        output_rollout,
        gate_rollout,
        up_rollout,
        down_rollout,
    ) = rollout
    widened = hidden.astype(jnp.float32)
    squares = jnp.sum(widened * widened, axis=1)
    joined = jnp.concatenate([query_rollout, key_rollout, value_rollout], axis=1)
    partial_value = jnp.dot(hidden, joined, preferred_element_type=jnp.float32)
    summed, total_sq = (
        lax.psum_scatter(partial_value, "fsdp", scatter_dimension=0, tiled=True),
        lax.psum_scatter(squares, "fsdp", scatter_dimension=0, tiled=True),
    )
    inv_rms = lax.rsqrt(total_sq / D + norm_eps)[:, None]
    width_q = query_rollout.shape[1]
    width_k = key_rollout.shape[1]
    query = summed[:, :width_q] * inv_rms / factors[0]
    key_new = summed[:, width_q : width_q + width_k] * inv_rms / factors[1]
    value_new = summed[:, width_q + width_k :] * inv_rms / factors[2]
    count_seq = summed.shape[0]
    query = rotate(query.reshape(count_seq, -1, HEAD_DIM), lengths).astype(jnp.bfloat16)
    query = query.reshape(count_seq, -1, HEADS // KV_HEADS, HEAD_DIM)
    key_new = rotate(key_new.reshape(count_seq, -1, HEAD_DIM), lengths).astype(jnp.bfloat16)
    value_new = value_new.reshape(count_seq, -1, HEAD_DIM).astype(jnp.bfloat16)
    attention_out = attend(query, key_new, value_new, key_cache, value_cache, lengths)
    return (
        attention_out,
        query_rollout,
        key_rollout,
        value_rollout,
        output_rollout,
        gate_rollout,
        up_rollout,
        down_rollout,
        new_history,
    )


LANES = 128


def fits(mesh, arrays):
    shards, half = mesh.shape["fsdp"], mesh.shape["tp"]
    width = arrays[0].shape[1] // shards
    if shards & (shards - 1) or shards < 4 or width % LANES != LANES // 2:
        return False
    counts = [w.shape[1] // (shards * half) for w in (arrays[1], arrays[2], arrays[3], arrays[5])]
    return all(c % 32 == 0 and (4 * c) % LANES == 0 for c in counts)


def pack_kernel(counts, span, extra_mode, me_ref, *refs):
    ins = refs[: len(counts)]
    refs = refs[len(counts) :]
    if extra_mode:
        extra, refs = refs[0], refs[1:]
    outs, (buf, sems, extra_sems) = refs[:-3], refs[-3:]
    step = pl.program_id(0)
    steps = len(outs) // 2
    slot = lax.rem(step, 2)
    side = lax.rem(me_ref[0], 2)
    bulk = sum(c * span // LANES for c in counts)
    lead = span // LANES

    def drain(where):
        for part in range(2):
            pltpu.make_async_copy(
                buf.at[where, part], outs[0].at[pl.ds(0, bulk)], sems.at[where, part]
            ).wait()

    @pl.when(step >= 2)
    def _():
        drain(slot)

    base = 0
    for ref, count in zip(ins, counts):
        half = count // 2
        for tile in range(lead):
            buf[slot, 0, pl.ds(base + tile * count, count)] = ref[
                :, tile * LANES : (tile + 1) * LANES
            ]
            buf[slot, 1, pl.ds(base + tile * count, count)] = ref[
                :, (tile + lead + 1) * LANES : (tile + lead + 2) * LANES
            ]
        shared = ref[:, lead * LANES : (lead + 1) * LANES].astype(jnp.float32)
        low, high = shared[:half], shared[half:]
        left = lax.broadcasted_iota(jnp.int32, (half, LANES), 1) < LANES // 2
        tail = base + lead * count
        buf[slot, 0, pl.ds(tail, half)] = jnp.where(
            left, low, pltpu.roll(high, LANES // 2, 1)
        ).astype(jnp.bfloat16)
        buf[slot, 1, pl.ds(tail, half)] = jnp.where(
            left, pltpu.roll(low, LANES // 2, 1), high
        ).astype(jnp.bfloat16)
        base += count * span // LANES

    first = me_ref[1]
    for index in range(steps):

        @pl.when(step == index)
        def _():
            for part in range(2):
                out = outs[2 * index + part]
                pltpu.make_async_copy(
                    buf.at[slot, side if part == 0 else 1 - side],
                    out.at[pl.ds(0, bulk)],
                    sems.at[slot, part],
                ).start()
                if extra_mode:
                    height = extra.shape[-2]
                    peer = me_ref[0] ^ (2 * (first + index) + part)
                    source = extra if extra_mode == 1 else extra.at[peer]
                    pltpu.make_async_copy(
                        source, out.at[pl.ds(bulk, height)], extra_sems.at[index, part]
                    ).start()

    @pl.when(step == steps - 1)
    def _():
        if steps > 1:
            drain(1 - slot)
        drain(slot)
        if extra_mode:
            height = extra.shape[-2]
            source = extra if extra_mode == 1 else extra.at[0]
            for index in range(steps):
                for part in range(2):
                    pltpu.make_async_copy(
                        source,
                        outs[0].at[pl.ds(bulk, height)],
                        extra_sems.at[index, part],
                    ).wait()


def pack(tensors, me, shards, first, steps, extra=None):
    span = tensors[0].shape[1] // shards
    counts = [t.shape[0] for t in tensors]
    bulk = sum(c * span // LANES for c in counts)
    mode = 0 if extra is None else extra.ndim - 1
    rows = bulk + (0 if extra is None else extra.shape[-2])
    spot = jnp.stack([me, jnp.int32(first)])

    def block(step, spot):
        return (0, (spot[0] // 2) ^ (spot[1] + step))

    in_specs = [pl.BlockSpec((c, 2 * span), block) for c in counts]
    operands = list(tensors)
    if mode:
        in_specs.append(pl.BlockSpec(memory_space=pltpu.VMEM))
        operands.append(extra)
    moved = sum(t.size for t in tensors) * 2 * steps // (shards // 2)
    return pl.pallas_call(
        functools.partial(pack_kernel, counts, span, mode),
        grid_spec=pltpu.PrefetchScalarGridSpec(
            num_scalar_prefetch=1,
            grid=(steps,),
            in_specs=in_specs,
            out_specs=[pl.BlockSpec(memory_space=pl.ANY)] * (2 * steps),
            scratch_shapes=[
                pltpu.VMEM((2, 2, bulk, LANES), jnp.bfloat16),
                pltpu.SemaphoreType.DMA((2, 2)),
                pltpu.SemaphoreType.DMA((steps, 2)),
            ],
        ),
        out_shape=[jax.ShapeDtypeStruct((rows, LANES), jnp.bfloat16)] * (2 * steps),
        compiler_params=pltpu.CompilerParams(dimension_semantics=("arbitrary",)),
        cost_estimate=pl.CostEstimate(
            flops=moved * 200, bytes_accessed=2 * moved, transcendentals=0
        ),
        name="pack",
    )(spot, *operands)


def unpack_kernel(count, span, start, shards, me_ref, factor_ref, *refs):
    chunks = refs[:shards]
    out, whole, shared, sems = refs[shards:]
    group = pl.program_id(0)
    me = me_ref[0]
    side = lax.rem(me, 2)
    lead = span // LANES
    half = count // 2

    def copies(chunk, source):
        at = pl.multiple_of(source * count, 32)
        made = [
            pltpu.make_async_copy(
                chunk.at[pl.ds(start + tile * count, count)],
                whole.at[tile, pl.ds(at, count)],
                sems.at[source, tile],
            )
            for tile in range(lead)
        ]
        for part in range(2):
            made.append(
                pltpu.make_async_copy(
                    chunk.at[pl.ds(start + lead * count, half)],
                    shared.at[pl.ds(at + part * half, half)],
                    sems.at[source, lead + part],
                )
            )
        return made

    @pl.when(group == 0)
    def _():
        for number in range(shards):
            for copy in copies(chunks[number], me ^ number):
                copy.start()

    for member in range(4):
        for copy in copies(chunks[0], group * 4 + member):
            copy.wait()

    factor = factor_ref[0]
    rise = pl.multiple_of(side * (LANES // 2), LANES // 2)
    fall = pl.multiple_of((1 - side) * (lead * LANES), LANES // 2)

    def tile_step(tile, carry):
        row = pl.multiple_of(group * (4 * count) + tile * LANES, LANES)
        column = pl.ds(pl.multiple_of(tile * LANES, LANES), LANES)
        for number in range(lead):
            piece = whole[number, pl.ds(row, LANES), :].astype(jnp.float32)
            out[pl.ds(pl.multiple_of(rise + number * LANES, LANES // 2), LANES), column] = (
                piece.T * factor
            ).astype(jnp.bfloat16)
        piece = shared[pl.ds(row, LANES), :].astype(jnp.float32).T
        spot = row + lax.broadcasted_iota(jnp.int32, (LANES // 2, LANES), 1)
        low = lax.rem(spot, count) < half
        out[pl.ds(fall, LANES // 2), column] = (
            jnp.where(low, piece[: LANES // 2], piece[LANES // 2 :]) * factor
        ).astype(jnp.bfloat16)
        return carry

    lax.fori_loop(0, 4 * count // LANES, tile_step, 0)


def unpack(chunks, me, factor, count, span, start):
    shards = len(chunks)
    size = shards * count * span
    return pl.pallas_call(
        functools.partial(unpack_kernel, count, span, start, shards),
        grid_spec=pltpu.PrefetchScalarGridSpec(
            num_scalar_prefetch=2,
            grid=(shards // 4,),
            in_specs=[pl.BlockSpec(memory_space=pl.ANY)] * shards,
            out_specs=pl.BlockSpec((span, 4 * count), lambda group, me, factor: (0, group)),
            scratch_shapes=[
                pltpu.VMEM((span // LANES, shards * count, LANES), jnp.bfloat16),
                pltpu.VMEM((shards * count, LANES), jnp.bfloat16),
                pltpu.SemaphoreType.DMA((shards, span // LANES + 2)),
            ],
        ),
        out_shape=jax.ShapeDtypeStruct((span, shards * count), jnp.bfloat16),
        compiler_params=pltpu.CompilerParams(dimension_semantics=("arbitrary",)),
        cost_estimate=pl.CostEstimate(
            flops=size * 200, bytes_accessed=4 * size, transcendentals=0
        ),
        name="unpack",
    )(me.reshape(1), factor.reshape(1), *chunks)


def collect_kernel(start, height, me_ref, *refs):
    chunks, out, sems = refs[:-2], refs[-2], refs[-1]

    def copy(number):
        return pltpu.make_async_copy(
            chunks[number].at[pl.ds(start, height)], out.at[me_ref[0] ^ number], sems.at[number]
        )

    for number in range(len(chunks)):
        copy(number).start()
    for number in range(len(chunks)):
        copy(number).wait()


def collect(chunks, me, start, height):
    shards = len(chunks)
    return pl.pallas_call(
        functools.partial(collect_kernel, start, height),
        grid_spec=pltpu.PrefetchScalarGridSpec(
            num_scalar_prefetch=1,
            grid=(1,),
            in_specs=[pl.BlockSpec(memory_space=pl.ANY)] * shards,
            out_specs=pl.BlockSpec((shards, height, LANES), lambda step, me: (0, 0, 0)),
            scratch_shapes=[pltpu.SemaphoreType.DMA((shards,))],
        ),
        out_shape=jax.ShapeDtypeStruct((shards, height, LANES), jnp.bfloat16),
        cost_estimate=pl.CostEstimate(
            flops=1 << 20, bytes_accessed=shards * height * LANES * 4, transcendentals=0
        ),
        name="collect",
    )(me.reshape(1), *chunks)


def exchange(chunks, order):
    shards = len(chunks)
    arrived = list(chunks)
    for number in order:
        pairs = [(source, source ^ number) for source in range(shards)]
        arrived[number] = lax.ppermute(chunks[number], "fsdp", pairs)
    return arrived


def after(token, *values):
    return lax.optimization_barrier((token, *values))[1:]


def three_terms(values):
    terms = []
    for _ in range(3):
        term = lax.reduce_precision(values, 8, 7)
        terms.append(term.astype(jnp.bfloat16))
        values = values - term
    return jnp.stack(terms, axis=1)


def packed_step(
    shards,
    half,
    hidden,
    query_weight,
    key_weight,
    value_weight,
    output_weight,
    gate_weight,
    up_weight,
    down_weight,
    history,
    slot,
    lengths,
    key_cache,
    value_cache,
):
    me = lax.axis_index("fsdp").astype(jnp.int32)
    span = hidden.shape[1]
    seqs = hidden.shape[0]
    share = seqs // shards
    query_t, key_t, value_t = query_weight.T, key_weight.T, value_weight.T
    gate_t, up_t = gate_weight.T, up_weight.T
    cross = shards // 2
    mixed = [cross]
    for number in range(1, cross):
        mixed += [number, cross + number]
    pairs = shards // 2

    def rows(tensor):
        return tensor.shape[0] * span // LANES

    wire_hidden = hidden.reshape(seqs * span // LANES, LANES)
    far = pack([gate_t], me, shards, pairs // 2, pairs // 2, wire_hidden)
    gate_near, hidden_near = after(far[0], gate_t, wire_hidden)
    near = pack([gate_near], me, shards, 0, pairs // 2, hidden_near)
    gate_chunks = near + far
    gate_chunks = exchange(gate_chunks, list(range(cross, shards)))
    gate_chunks = exchange(gate_chunks, list(range(1, cross)))

    trainer = (query_t, key_t, value_t, output_weight, gate_t, up_t, down_weight)
    staged = after(near[0], *trainer)
    local = jnp.stack([largest(tensor) for tensor in staged])
    tile = jnp.broadcast_to(jnp.pad(local, (0, 9))[:, None], (16, LANES)).astype(jnp.bfloat16)
    best = tile
    for turn in range(1, half):
        ring = [(source, (source + turn) % half) for source in range(half)]
        best = jnp.maximum(best, lax.ppermute(tile, "tp", ring))
    up_chunks = pack([up_t], me, shards, 0, pairs, best)
    (down_late,) = after(up_chunks[0], down_weight)
    down_chunks = pack([down_late], me, shards, 0, pairs)
    up_chunks = exchange(up_chunks, mixed)
    down_chunks = exchange(down_chunks, mixed)

    everyone = collect(gate_chunks, me, rows(gate_t), wire_hidden.shape[0])
    everyone = everyone.reshape(shards, seqs, span).transpose(1, 0, 2).reshape(seqs, shards * span)
    widened = everyone.astype(jnp.float32)
    inv_rms = lax.rsqrt(jnp.sum(widened * widened, axis=1) / D + norm_eps)[:, None]

    seen = collect(up_chunks, me, rows(up_t), best.shape[0])
    peaks = jnp.max(seen[:, :7, 0].astype(jnp.float32), axis=0)
    factors, new_history = scaling(peaks, history, slot)

    parts = []
    for number, tensor in enumerate((query_t, key_t, value_t)):
        product = lax.dot_general(
            everyone,
            quantize(tensor, factors[number]),
            (((1,), (1,)), ((), ())),
            preferred_element_type=jnp.float32,
        )
        parts.append(product * inv_rms / factors[number])
    joined = jnp.concatenate(parts, axis=1)
    width = joined.shape[1]
    padded = -(-width // LANES) * LANES
    terms = three_terms(jnp.pad(joined, ((0, 0), (0, padded - width))))
    terms = terms.reshape(shards, share, 3, padded // LANES, LANES)
    terms = terms.reshape(shards, share * 3 * padded // LANES, LANES)
    used = terms.shape[1]
    filled = -(-used // 16) * 16
    terms = jnp.pad(terms, ((0, 0), (0, filled - used), (0, 0)))
    output_chunks = pack([output_weight], me, shards, 0, pairs, terms)
    query_late, key_late, value_late = after(output_chunks[0], query_t, key_t, value_t)
    last = pack([query_late, key_late, value_late], me, shards, 0, pairs)
    output_chunks = exchange(output_chunks, mixed)
    last = exchange(last, mixed)

    mine = collect(output_chunks, me, rows(output_weight), filled)[:, :used]
    mine = mine.reshape(shards, share, 3, padded).astype(jnp.float32)
    mine = (mine[:, :, 2] + mine[:, :, 1] + mine[:, :, 0]).transpose(1, 0, 2)
    width_q, width_k = query_t.shape[0], key_t.shape[0]
    query = mine[:, :, :width_q].reshape(share, shards * width_q)
    key_new = mine[:, :, width_q : width_q + width_k].reshape(share, shards * width_k)
    value_new = mine[:, :, width_q + width_k : width].reshape(share, -1)
    query = rotate(query.reshape(share, -1, HEAD_DIM), lengths).astype(jnp.bfloat16)
    query = query.reshape(share, -1, HEADS // KV_HEADS, HEAD_DIM)
    key_new = rotate(key_new.reshape(share, -1, HEAD_DIM), lengths).astype(jnp.bfloat16)
    value_new = value_new.reshape(share, -1, HEAD_DIM).astype(jnp.bfloat16)
    attention_out = attend(query, key_new, value_new, key_cache, value_cache, lengths)

    def finish(chunks, number, tensor, start=0):
        return unpack(chunks, me, factors[number], tensor.shape[0], span, start)

    return (
        attention_out,
        finish(last, 0, query_t),
        finish(last, 1, key_t, rows(query_t)),
        finish(last, 2, value_t, rows(query_t) + rows(key_t)),
        finish(output_chunks, 3, output_weight).T,
        finish(gate_chunks, 4, gate_t),
        finish(up_chunks, 5, up_t),
        finish(down_chunks, 6, down_weight).T,
        new_history,
    )


def solution(mesh):
    return lambda *arrays: build(mesh, arrays)(*arrays)


def build(mesh, arrays):
    shards, half = mesh.shape["fsdp"], mesh.shape["tp"]
    if fits(mesh, arrays):
        return sharded(mesh, functools.partial(packed_step, shards, half))
    return sharded(mesh, general_step)


def sharded(mesh, body):
    return jax.shard_map(
        body,
        mesh=mesh,
        in_specs=(
            P(None, "fsdp"),
            P(None, ("tp", "fsdp")),
            P(None, ("tp", "fsdp")),
            P(None, ("tp", "fsdp")),
            P(("tp", "fsdp"), None),
            P(None, ("tp", "fsdp")),
            P(None, ("tp", "fsdp")),
            P(("tp", "fsdp"), None),
            P(),
            P(),
            P("fsdp"),
            P("fsdp", None, "tp"),
            P("fsdp", None, "tp"),
        ),
        out_specs=(
            P("fsdp", "tp"),
            P("fsdp", "tp"),
            P("fsdp", "tp"),
            P("fsdp", "tp"),
            P("tp", "fsdp"),
            P("fsdp", "tp"),
            P("fsdp", "tp"),
            P("tp", "fsdp"),
            P(),
        ),
        check_vma=False,
    )
```

```python
import functools

import jax
import jax.numpy as jnp
from jax import lax
from jax.experimental import pallas as pl
from jax.experimental.pallas import tpu as pltpu
from jax.sharding import PartitionSpec as P


D = 5120
HEADS = 40
KV_HEADS = 8
HEAD_DIM = 128


target_peak = 4.0
norm_eps = 1e-06
rope_theta = 1000000.0


def largest(tensor):
    return jnp.max(jnp.abs(tensor.astype(jnp.float32)))


def scaling(peaks, history, slot):
    marked = lax.broadcasted_iota(jnp.int32, history.shape, 1) == slot[0]
    kept = jnp.max(jnp.where(marked, jnp.zeros_like(history), history), axis=1)
    return (target_peak / jnp.maximum(peaks, kept), jnp.where(marked, peaks[:, None], history))


def quantize(tensor, factor):
    return (tensor.astype(jnp.float32) * factor).astype(jnp.bfloat16)


def rotate(vectors, positions):
    half_dim = vectors.shape[-1] // 2
    ladder = jnp.arange(half_dim, dtype=jnp.float32)
    spread = rope_theta ** (-2.0 * ladder / vectors.shape[-1])
    angle = positions.astype(jnp.float32)[:, None] * spread[None, :]
    cosine = jnp.cos(angle)[:, None, :]
    sine = jnp.sin(angle)[:, None, :]
    first = vectors[..., :half_dim]
    second = vectors[..., half_dim:]
    return jnp.concatenate(
        [first * cosine - second * sine, second * cosine + first * sine], axis=-1
    )


def regroup(query_part, key_part, value_part, output_part, gate_part, up_part, down_part):
    columns = (
        lax.all_to_all(query_part, "fsdp", split_axis=0, concat_axis=1, tiled=True),
        lax.all_to_all(key_part, "fsdp", split_axis=0, concat_axis=1, tiled=True),
        lax.all_to_all(value_part, "fsdp", split_axis=0, concat_axis=1, tiled=True),
        lax.all_to_all(gate_part, "fsdp", split_axis=0, concat_axis=1, tiled=True),
        lax.all_to_all(up_part, "fsdp", split_axis=0, concat_axis=1, tiled=True),
    )
    rowwise = (
        lax.all_to_all(output_part, "fsdp", split_axis=1, concat_axis=0, tiled=True),
        lax.all_to_all(down_part, "fsdp", split_axis=1, concat_axis=0, tiled=True),
    )
    return (columns[0], columns[1], columns[2], rowwise[0], columns[3], columns[4], rowwise[1])


def attend(query, key_new, value_new, key_cache, value_cache, lengths):
    count_seq = query.shape[0]
    kv_count = query.shape[1]
    head_dim = query.shape[3]
    cache_len = key_cache.shape[1]
    keys = key_cache.reshape(count_seq, cache_len, kv_count, head_dim)
    values = value_cache.reshape(count_seq, cache_len, kv_count, head_dim)
    scale = head_dim ** (-0.5)
    scores = jnp.einsum("bkgd,bjkd->bkgj", query, keys, preferred_element_type=jnp.float32) * scale
    own = (
        jnp.sum(query.astype(jnp.float32) * key_new.astype(jnp.float32)[:, :, None, :], axis=-1)
        * scale
    )
    valid = (lax.broadcasted_iota(jnp.int32, (count_seq, cache_len), 1) < lengths[:, None])[
        :, None, None, :
    ]
    top = jnp.maximum(jnp.max(jnp.where(valid, scores, -1e30), axis=-1), own)
    weights = jnp.where(valid, jnp.exp(scores - top[..., None]), 0.0)
    own_weight = jnp.exp(own - top)
    total = jnp.sum(weights, axis=-1) + own_weight
    probs = (weights / total[..., None]).astype(jnp.bfloat16)
    own_prob = (own_weight / total).astype(jnp.bfloat16)
    mixed = jnp.einsum("bkgj,bjkd->bkgd", probs, values, preferred_element_type=jnp.float32)
    mixed = (
        mixed
        + own_prob.astype(jnp.float32)[..., None] * value_new.astype(jnp.float32)[:, :, None, :]
    )
    return mixed.astype(jnp.bfloat16).reshape(count_seq, -1)


def general_step(
    hidden,
    query_weight,
    key_weight,
    value_weight,
    output_weight,
    gate_weight,
    up_weight,
    down_weight,
    history,
    slot,
    lengths,
    key_cache,
    value_cache,
):
    trainer = (
        query_weight,
        key_weight,
        value_weight,
        output_weight,
        gate_weight,
        up_weight,
        down_weight,
    )
    peaks = jnp.stack([lax.pmax(largest(tensor), ("fsdp", "tp")) for tensor in trainer])
    factors, new_history = scaling(peaks, history, slot)
    arrived = regroup(
        query_weight, key_weight, value_weight, output_weight, gate_weight, up_weight, down_weight
    )
    rollout = tuple((quantize(arrived[number], factors[number]) for number in range(7)))
    (
        query_rollout,
        key_rollout,
        value_rollout,
        output_rollout,
        gate_rollout,
        up_rollout,
        down_rollout,
    ) = rollout
    widened = hidden.astype(jnp.float32)
    squares = jnp.sum(widened * widened, axis=1)
    joined = jnp.concatenate([query_rollout, key_rollout, value_rollout], axis=1)
    partial_value = jnp.dot(hidden, joined, preferred_element_type=jnp.float32)
    summed, total_sq = (
        lax.psum_scatter(partial_value, "fsdp", scatter_dimension=0, tiled=True),
        lax.psum_scatter(squares, "fsdp", scatter_dimension=0, tiled=True),
    )
    inv_rms = lax.rsqrt(total_sq / D + norm_eps)[:, None]
    width_q = query_rollout.shape[1]
    width_k = key_rollout.shape[1]
    query = summed[:, :width_q] * inv_rms / factors[0]
    key_new = summed[:, width_q : width_q + width_k] * inv_rms / factors[1]
    value_new = summed[:, width_q + width_k :] * inv_rms / factors[2]
    count_seq = summed.shape[0]
    query = rotate(query.reshape(count_seq, -1, HEAD_DIM), lengths).astype(jnp.bfloat16)
    query = query.reshape(count_seq, -1, HEADS // KV_HEADS, HEAD_DIM)
    key_new = rotate(key_new.reshape(count_seq, -1, HEAD_DIM), lengths).astype(jnp.bfloat16)
    value_new = value_new.reshape(count_seq, -1, HEAD_DIM).astype(jnp.bfloat16)
    attention_out = attend(query, key_new, value_new, key_cache, value_cache, lengths)
    return (
        attention_out,
        query_rollout,
        key_rollout,
        value_rollout,
        output_rollout,
        gate_rollout,
        up_rollout,
        down_rollout,
        new_history,
    )


LANES = 128
UNROLL = 3


def fits(mesh, arrays):
    shards, half = mesh.shape["fsdp"], mesh.shape["tp"]
    width = arrays[0].shape[1] // shards
    if shards & (shards - 1) or shards < 4 or width % LANES != LANES // 2:
        return False
    counts = [w.shape[1] // (shards * half) for w in (arrays[1], arrays[2], arrays[3], arrays[5])]
    return all(c % 32 == 0 and (4 * c) % LANES == 0 for c in counts)


def pack_kernel(counts, span, first, extra_mode, waits, me_ref, *refs):
    ins = refs[: len(counts)]
    refs = refs[len(counts) :]
    if extra_mode:
        extra, refs = refs[0], refs[1:]
    refs = refs[waits:]
    outs, (buf, sems, extra_sems) = refs[:-3], refs[-3:]
    step = pl.program_id(0)
    steps = len(outs) // 2
    slot = lax.rem(step, 2)
    side = lax.rem(me_ref[0], 2)
    bulk = sum(c * span // LANES for c in counts)
    lead = span // LANES

    def drain(where):
        for part in range(2):
            pltpu.make_async_copy(
                buf.at[where, part], outs[0].at[pl.ds(0, bulk)], sems.at[where, part]
            ).wait()

    @pl.when(step >= 2)
    def _():
        drain(slot)

    base = 0
    for ref, count in zip(ins, counts):
        half = count // 2
        for tile in range(lead):
            buf[slot, 0, pl.ds(base + tile * count, count)] = ref[
                :, tile * LANES : (tile + 1) * LANES
            ]
            buf[slot, 1, pl.ds(base + tile * count, count)] = ref[
                :, (tile + lead + 1) * LANES : (tile + lead + 2) * LANES
            ]
        shared = ref[:, lead * LANES : (lead + 1) * LANES].astype(jnp.float32)
        low, high = shared[:half], shared[half:]
        left = lax.broadcasted_iota(jnp.int32, (half, LANES), 1) < LANES // 2
        tail = base + lead * count
        buf[slot, 0, pl.ds(tail, half)] = jnp.where(
            left, low, pltpu.roll(high, LANES // 2, 1)
        ).astype(jnp.bfloat16)
        buf[slot, 1, pl.ds(tail, half)] = jnp.where(
            left, pltpu.roll(low, LANES // 2, 1), high
        ).astype(jnp.bfloat16)
        base += count * span // LANES

    for index in range(steps):

        @pl.when(step == index)
        def _():
            for part in range(2):
                out = outs[2 * index + part]
                pltpu.make_async_copy(
                    buf.at[slot, side if part == 0 else 1 - side],
                    out.at[pl.ds(0, bulk)],
                    sems.at[slot, part],
                ).start()
                if extra_mode:
                    height = extra.shape[-2]
                    peer = me_ref[0] ^ (2 * (first + index) + part)
                    source = extra if extra_mode == 1 else extra.at[peer]
                    pltpu.make_async_copy(
                        source, out.at[pl.ds(bulk, height)], extra_sems.at[index, part]
                    ).start()

    @pl.when(step == steps - 1)
    def _():
        if steps > 1:
            drain(1 - slot)
        drain(slot)
        if extra_mode:
            height = extra.shape[-2]
            source = extra if extra_mode == 1 else extra.at[0]
            for index in range(steps):
                for part in range(2):
                    pltpu.make_async_copy(
                        source,
                        outs[0].at[pl.ds(bulk, height)],
                        extra_sems.at[index, part],
                    ).wait()


def pack(tensors, me, shards, first, steps, extra=None, wait=()):
    span = tensors[0].shape[1] // shards
    counts = [t.shape[0] for t in tensors]
    bulk = sum(c * span // LANES for c in counts)
    mode = 0 if extra is None else extra.ndim - 1
    rows = bulk + (0 if extra is None else extra.shape[-2])

    def block(step, me):
        return (0, (me[0] // 2) ^ (first + step))

    in_specs = [pl.BlockSpec((c, 2 * span), block) for c in counts]
    operands = list(tensors)
    if mode:
        in_specs.append(pl.BlockSpec(memory_space=pltpu.VMEM))
        operands.append(extra)
    in_specs += [pl.BlockSpec(memory_space=pl.ANY)] * len(wait)
    operands += list(wait)
    moved = sum(t.size for t in tensors) * 2 * steps // (shards // 2)
    return pl.pallas_call(
        functools.partial(pack_kernel, counts, span, first, mode, len(wait)),
        grid_spec=pltpu.PrefetchScalarGridSpec(
            num_scalar_prefetch=1,
            grid=(steps,),
            in_specs=in_specs,
            out_specs=[pl.BlockSpec(memory_space=pl.ANY)] * (2 * steps),
            scratch_shapes=[
                pltpu.VMEM((2, 2, bulk, LANES), jnp.bfloat16),
                pltpu.SemaphoreType.DMA((2, 2)),
                pltpu.SemaphoreType.DMA((steps, 2)),
            ],
        ),
        out_shape=[jax.ShapeDtypeStruct((rows, LANES), jnp.bfloat16)] * (2 * steps),
        compiler_params=pltpu.CompilerParams(dimension_semantics=("arbitrary",)),
        cost_estimate=pl.CostEstimate(
            flops=moved * 200, bytes_accessed=2 * moved, transcendentals=0
        ),
        name="pack",
    )(me.reshape(1), *operands)


def unpack_kernel(count, span, start, shards, me_ref, factor_ref, *refs):
    chunks = refs[:shards]
    out, landed, whole, shared, sems = refs[shards:]
    group = pl.program_id(0)
    me = me_ref[0]
    side = lax.rem(me, 2)
    lead = span // LANES
    half = count // 2
    height = count * span // LANES

    def copy(chunk, source):
        return pltpu.make_async_copy(
            chunk.at[pl.ds(start, height)], landed.at[source], sems.at[source]
        )

    @pl.when(group == 0)
    def _():
        for number in range(shards):
            copy(chunks[number], me ^ number).start()

    for member in range(4):
        source = group * 4 + member
        copy(chunks[0], source).wait()
        for number in range(lead):
            whole[number, pl.ds(member * count, count)] = landed[
                source, pl.ds(number * count, count)
            ]
        tail = landed[source, pl.ds(lead * count, half)]
        shared[pl.ds(member * count, half)] = tail
        shared[pl.ds(member * count + half, half)] = tail

    factor = factor_ref[0]
    rise = pl.multiple_of(side * (LANES // 2), LANES // 2)
    fall = pl.multiple_of((1 - side) * (lead * LANES), LANES // 2)

    def tile_step(tile, carry):
        row = pl.multiple_of(tile * LANES, LANES)
        column = pl.ds(row, LANES)
        for number in range(lead):
            piece = whole[number, pl.ds(row, LANES), :].T.astype(jnp.float32)
            out[pl.ds(pl.multiple_of(rise + number * LANES, LANES // 2), LANES), column] = (
                piece * factor
            ).astype(jnp.bfloat16)
        piece = shared[pl.ds(row, LANES), :].T.astype(jnp.float32)
        spot = row + lax.broadcasted_iota(jnp.int32, (LANES // 2, LANES), 1)
        low = lax.rem(spot, count) < half
        out[pl.ds(fall, LANES // 2), column] = (
            jnp.where(low, piece[: LANES // 2], piece[LANES // 2 :]) * factor
        ).astype(jnp.bfloat16)
        return carry

    lax.fori_loop(0, 4 * count // LANES, tile_step, 0, unroll=UNROLL)


def unpack(chunks, me, factor, count, span, start):
    shards = len(chunks)
    size = shards * count * span
    return pl.pallas_call(
        functools.partial(unpack_kernel, count, span, start, shards),
        grid_spec=pltpu.PrefetchScalarGridSpec(
            num_scalar_prefetch=2,
            grid=(shards // 4,),
            in_specs=[pl.BlockSpec(memory_space=pl.ANY)] * shards,
            out_specs=pl.BlockSpec((span, 4 * count), lambda group, me, factor: (0, group)),
            scratch_shapes=[
                pltpu.VMEM((shards, count * span // LANES, LANES), jnp.bfloat16),
                pltpu.VMEM((span // LANES, 4 * count, LANES), jnp.bfloat16),
                pltpu.VMEM((4 * count, LANES), jnp.bfloat16),
                pltpu.SemaphoreType.DMA((shards,)),
            ],
        ),
        out_shape=jax.ShapeDtypeStruct((span, shards * count), jnp.bfloat16),
        compiler_params=pltpu.CompilerParams(dimension_semantics=("arbitrary",)),
        cost_estimate=pl.CostEstimate(
            flops=size * 200, bytes_accessed=4 * size, transcendentals=0
        ),
        name="unpack",
    )(me.reshape(1), factor.reshape(1), *chunks)


def collect_kernel(places, height, me_ref, *refs):
    chunks, out, sems = refs[:-2], refs[-2], refs[-1]
    copies = [
        pltpu.make_async_copy(
            chunks[chunk].at[pl.ds(start, height)], out.at[me_ref[0] ^ number], sems.at[number]
        )
        for number, (chunk, start) in enumerate(places)
    ]
    for copy in copies:
        copy.start()
    for copy in copies:
        copy.wait()


def collect(chunks, me, places, height):
    shards = len(places)
    return pl.pallas_call(
        functools.partial(collect_kernel, places, height),
        grid_spec=pltpu.PrefetchScalarGridSpec(
            num_scalar_prefetch=1,
            grid=(1,),
            in_specs=[pl.BlockSpec(memory_space=pl.ANY)] * len(chunks),
            out_specs=pl.BlockSpec((shards, height, LANES), lambda step, me: (0, 0, 0)),
            scratch_shapes=[pltpu.SemaphoreType.DMA((shards,))],
        ),
        out_shape=jax.ShapeDtypeStruct((shards, height, LANES), jnp.bfloat16),
        cost_estimate=pl.CostEstimate(
            flops=1 << 20, bytes_accessed=shards * height * LANES * 4, transcendentals=0
        ),
        name="collect",
    )(me.reshape(1), *chunks)


def exchange(chunks, order):
    shards = lax.axis_size("fsdp")
    arrived = list(chunks)
    for number in order:
        pairs = [(source, source ^ number) for source in range(shards)]
        arrived[number] = lax.ppermute(chunks[number], "fsdp", pairs)
    return arrived


def after(token, *values):
    return lax.optimization_barrier((token, *values))[1:]


def three_terms(values):
    terms = []
    for _ in range(3):
        term = lax.reduce_precision(values, 8, 7)
        terms.append(term.astype(jnp.bfloat16))
        values = values - term
    return jnp.stack(terms, axis=1)


def packed_step(
    shards,
    half,
    hidden,
    query_weight,
    key_weight,
    value_weight,
    output_weight,
    gate_weight,
    up_weight,
    down_weight,
    history,
    slot,
    lengths,
    key_cache,
    value_cache,
):
    me = lax.axis_index("fsdp").astype(jnp.int32)
    span = hidden.shape[1]
    seqs = hidden.shape[0]
    share = seqs // shards
    query_t, key_t, value_t = query_weight.T, key_weight.T, value_weight.T
    gate_t, up_t = gate_weight.T, up_weight.T
    cross = shards // 2
    pairs = shards // 2
    mixed = [cross]
    for number in range(1, cross):
        mixed += [number, cross + number]

    def rows(tensor):
        return tensor.shape[0] * span // LANES

    far, near = range(cross, shards), range(1, cross)
    lower, fourth = pairs // 2, pairs // 4
    height = seqs * span // LANES
    gate_far = pack([gate_t], me, shards, lower, fourth)
    (hidden_late,) = after(gate_far[0], hidden)
    own_hidden = hidden_late.reshape(height, LANES)
    other_hidden = exchange([own_hidden] * shards, [cross])[cross]

    trainer = (query_t, key_t, value_t, output_weight, gate_t, up_t, down_weight)
    staged = after(gate_far[0], *trainer)
    local = jnp.stack([largest(tensor) for tensor in staged])
    tile = jnp.broadcast_to(jnp.pad(local, (0, 9))[:, None], (16, LANES)).astype(jnp.bfloat16)
    best = tile
    for turn in range(1, half):
        ring = [(source, (source + turn) % half) for source in range(half)]
        best = jnp.maximum(best, lax.ppermute(tile, "tp", ring))
    low = best.shape[0]
    pair_far = pack([key_t, value_t], me, shards, lower, lower, best)
    key_late, value_late = after(pair_far[0], key_t, value_t)
    both = jnp.concatenate([best, own_hidden, other_hidden], axis=0)
    pair_near = pack([key_late, value_late], me, shards, 0, lower, both)
    pair_chunks = pair_near + pair_far
    pair_chunks = exchange(pair_chunks, far)
    pair_chunks = exchange(pair_chunks, near)
    (gate_two,) = after(pair_near[0], gate_t)
    gate_far += pack([gate_two], me, shards, lower + fourth, lower - fourth)
    (gate_two,) = after(gate_far[-1], gate_t)
    gate_near = pack([gate_two], me, shards, 0, lower)
    gate_chunks = gate_near + gate_far
    split = cross + 2 * fourth
    gate_chunks = exchange(gate_chunks, range(cross, cross + 1))
    gate_chunks = exchange(gate_chunks, range(cross + 1, split))
    gate_chunks = exchange(gate_chunks, range(split, shards))
    gate_chunks = exchange(gate_chunks, near)

    bulk = rows(key_t) + rows(value_t)
    seen = collect(pair_chunks, me, [(number, bulk) for number in range(shards)], low)
    peaks = jnp.max(seen[:, :7, 0].astype(jnp.float32), axis=0)
    factors, new_history = scaling(peaks, history, slot)
    places = [(number % cross, bulk + low + number // cross * height) for number in range(shards)]
    everyone = collect(pair_chunks[:cross], me, places, height)
    everyone = everyone.reshape(shards, seqs, span).transpose(1, 0, 2).reshape(seqs, shards * span)
    widened = everyone.astype(jnp.float32)
    inv_rms = lax.rsqrt(jnp.sum(widened * widened, axis=1) / D + norm_eps)[:, None]

    parts = []
    for number, tensor in enumerate((query_t, key_t, value_t)):
        product = lax.dot_general(
            everyone,
            quantize(tensor, factors[number]),
            (((1,), (1,)), ((), ())),
            preferred_element_type=jnp.float32,
        )
        parts.append(product * inv_rms / factors[number])
    joined = jnp.concatenate(parts, axis=1)
    width = joined.shape[1]
    padded = -(-width // LANES) * LANES
    terms = three_terms(jnp.pad(joined, ((0, 0), (0, padded - width))))
    terms = terms.reshape(shards, share, 3, padded // LANES, LANES)
    terms = terms.reshape(shards, share * 3 * padded // LANES, LANES)
    used = terms.shape[1]
    filled = -(-used // 16) * 16
    terms = jnp.pad(terms, ((0, 0), (0, filled - used), (0, 0)))
    up_chunks = pack([up_t, query_t], me, shards, 0, pairs, terms)
    up_chunks = exchange(up_chunks, mixed)
    down_chunks = pack([down_weight], me, shards, 0, pairs, None, gate_chunks[1:])
    down_chunks = exchange(down_chunks, mixed)
    places = [(number, rows(up_t) + rows(query_t)) for number in range(shards)]
    mine = collect(up_chunks, me, places, filled)
    output_chunks = pack([output_weight], me, shards, 0, pairs, None, (mine,))
    output_chunks = exchange(output_chunks, mixed)
    mine = mine[:, :used]
    mine = mine.reshape(shards, share, 3, padded).astype(jnp.float32)
    mine = (mine[:, :, 2] + mine[:, :, 1] + mine[:, :, 0]).transpose(1, 0, 2)
    width_q, width_k = query_t.shape[0], key_t.shape[0]
    query = mine[:, :, :width_q].reshape(share, shards * width_q)
    key_new = mine[:, :, width_q : width_q + width_k].reshape(share, shards * width_k)
    value_new = mine[:, :, width_q + width_k : width].reshape(share, -1)
    query = rotate(query.reshape(share, -1, HEAD_DIM), lengths).astype(jnp.bfloat16)
    query = query.reshape(share, -1, HEADS // KV_HEADS, HEAD_DIM)
    key_new = rotate(key_new.reshape(share, -1, HEAD_DIM), lengths).astype(jnp.bfloat16)
    value_new = value_new.reshape(share, -1, HEAD_DIM).astype(jnp.bfloat16)
    attention_out = attend(query, key_new, value_new, key_cache, value_cache, lengths)

    def finish(chunks, number, tensor, start=0):
        return unpack(chunks, me, factors[number], tensor.shape[0], span, start)

    return (
        attention_out,
        finish(up_chunks, 0, query_t, rows(up_t)),
        finish(pair_chunks, 1, key_t),
        finish(pair_chunks, 2, value_t, rows(key_t)),
        finish(output_chunks, 3, output_weight).T,
        finish(gate_chunks, 4, gate_t),
        finish(up_chunks, 5, up_t),
        finish(down_chunks, 6, down_weight).T,
        new_history,
    )


def solution(mesh):
    return lambda *arrays: build(mesh, arrays)(*arrays)


def build(mesh, arrays):
    shards, half = mesh.shape["fsdp"], mesh.shape["tp"]
    if fits(mesh, arrays):
        return sharded(mesh, functools.partial(packed_step, shards, half))
    return sharded(mesh, general_step)


def sharded(mesh, body):
    return jax.shard_map(
        body,
        mesh=mesh,
        in_specs=(
            P(None, "fsdp"),
            P(None, ("tp", "fsdp")),
            P(None, ("tp", "fsdp")),
            P(None, ("tp", "fsdp")),
            P(("tp", "fsdp"), None),
            P(None, ("tp", "fsdp")),
            P(None, ("tp", "fsdp")),
            P(("tp", "fsdp"), None),
            P(),
            P(),
            P("fsdp"),
            P("fsdp", None, "tp"),
            P("fsdp", None, "tp"),
        ),
        out_specs=(
            P("fsdp", "tp"),
            P("fsdp", "tp"),
            P("fsdp", "tp"),
            P("fsdp", "tp"),
            P("tp", "fsdp"),
            P("fsdp", "tp"),
            P("fsdp", "tp"),
            P("tp", "fsdp"),
            P(),
        ),
        check_vma=False,
    )
```
